32 devices in a mesh: wide: 8 (over z, core), narrow: 4 (over y, x).
Axes of the slice: x: 2, y: 2, z: 4, core: 2. Of those that a mesh axis runs over, the one named last changes fastest.
Arguments:
- hidden_in: bfloat16 [2, 32, 512, 1024], P(None, ('wide', 'narrow')), may hold values from -6 to 6
- segment_ids: int32 [2, 32, 512], P(None, ('wide', 'narrow')), may hold values from 0 to 7, never falling along the last dimension, each value on 1 to 128 neighbouring positions
- bucket_ids: int32 [1023], replicated, may hold values from 0 to 31
- norm1_gain: bfloat16 [1024], P(('wide', 'narrow')), may hold values from 0.5 to 1.5
- rel_bias: bfloat16 [512], P(('wide', 'narrow')), may hold values from -4 to 4
- query_weight: bfloat16 [1024, 1024], P(('wide', 'narrow')), may hold values from -0.046875 to 0.046875
- key_weight: bfloat16 [1024, 1024], P(('wide', 'narrow')), may hold values from -0.1875 to 0.1875
- value_weight: bfloat16 [1024, 1024], P(('wide', 'narrow')), may hold values from -0.1875 to 0.1875
- output_weight: bfloat16 [1024, 1024], P(('wide', 'narrow')), may hold values from -0.75 to 0.75
- norm2_gain: bfloat16 [1024], P(('wide', 'narrow')), may hold values from 0.5 to 1.5
- gate_weight: bfloat16 [1024, 2816], P(('wide', 'narrow')), may hold values from -0.1875 to 0.1875
- up_weight: bfloat16 [1024, 2816], P(('wide', 'narrow')), may hold values from -0.1875 to 0.1875
- down_weight: bfloat16 [2816, 1024], P(('wide', 'narrow')), may hold values from -0.109375 to 0.109375
- out_grad: bfloat16 [2, 32, 512, 1024], P(None, ('wide', 'narrow')), may hold values from -6 to 6
Outputs:
- hidden_out: bfloat16 [2, 32, 512, 1024], P(None, ('wide', 'narrow'))
- input_grad: bfloat16 [2, 32, 512, 1024], P(None, ('wide', 'narrow'))
- norm1_gain_grad: float32 [1024], P(('wide', 'narrow'))
- rel_bias_grad: float32 [512], P(('wide', 'narrow'))
- query_weight_grad: float32 [1024, 1024], P(('wide', 'narrow'))
- key_weight_grad: float32 [1024, 1024], P(('wide', 'narrow'))
- value_weight_grad: float32 [1024, 1024], P(('wide', 'narrow'))
- output_weight_grad: float32 [1024, 1024], P(('wide', 'narrow'))
- norm2_gain_grad: float32 [1024], P(('wide', 'narrow'))
- gate_weight_grad: float32 [1024, 2816], P(('wide', 'narrow'))
- up_weight_grad: float32 [1024, 2816], P(('wide', 'narrow'))
- down_weight_grad: float32 [2816, 1024], P(('wide', 'narrow'))
The draws below stay inside these ranges and needn't reach their ends.
All inputs are finite; a program needn't handle non-finite values.
Results may differ from the reference program's by a relative error of at most 0.014.
The reference program's roundings to bfloat16 on the way count: a program that leaves them out, or rounds other values in their place, can miss the bound.
Values may be sent and summed in bfloat16 or wider, within the bound.
A program may use at most 216 MiB of HBM per device.

```python
import math
import jax
import jax.numpy as jnp
import numpy as np
from jax import lax

D = 1024
H = 16
DH = 64
FF = 2816
BUCKETS = 32
SEQ = 512
MB = 2
SEQS = 32


def with_ends(drawn, rng, least, largest):
    dims = drawn.shape
    spot = [jax.random.randint(jax.random.fold_in(rng, axis), (), 0, dims[axis]) for axis in range(len(dims))]
    drawn = drawn.at[tuple(spot)].set(least)
    longest = dims.index(max(dims))
    spot[longest] = (spot[longest] + 1) % dims[longest]
    return drawn.at[tuple(spot)].set(largest)


def steps_of(own_key, dims, cuts, least, largest):
    level, own = 1.0, jax.random.fold_in(own_key, 6)
    for dim, parts in cuts:
        steps = jnp.exp(jax.random.uniform(jax.random.fold_in(own, dim), (parts,), jnp.float32, least / len(cuts), largest / len(cuts)))
        level = level * jnp.repeat(steps, dims[dim] // parts).reshape([-1 if axis == dim else 1 for axis in range(len(dims))])
    return level


def profile(number_of, total, limit, lean):
    portions = [(1 << 20) // math.isqrt(grade ** lean) + 1 for grade in range(2, number_of + 1)]
    rest, holding = total - limit - (number_of - 1), [1] * (number_of - 1)
    while rest > 0:
        movable = [i for i in range(number_of - 1) if holding[i] < limit]
        whole, left = sum([portions[i] for i in movable]), rest
        for i in movable:
            extra = min(limit - holding[i], max(1, left * portions[i] // whole), rest)
            holding[i] = holding[i] + extra
            rest = rest - extra
    return np.array([limit] + holding)


def uneven(key, amount, total, most, skew):
    if amount == 2:
        one = jax.random.randint(key, (), max(1, total - most), min(most, total - 1) + 1)
        return jnp.stack([one, total - one])
    lengths = jnp.asarray(profile(amount, total, most, skew), jnp.int32)
    pairs = (amount - 1) // 2
    giver, receiver = lengths[1:1 + 2 * pairs:2], lengths[2:2 + 2 * pairs:2]
    slack = jnp.minimum(giver - 1, most - receiver)
    moved = jax.random.randint(jax.random.fold_in(key, 1), (pairs,), 0, 1 << 20) % (slack + 1)
    lengths = lengths.at[1:1 + 2 * pairs:2].set(giver - moved).at[2:2 + 2 * pairs:2].set(receiver + moved)
    return lengths[jax.random.permutation(jax.random.fold_in(key, 2), amount)]


def gaussian(rng, dims, width, limit, cuts=(), kind=jnp.bfloat16):
    array = width * jax.random.normal(rng, dims, jnp.float32)
    if cuts:
        array = array * steps_of(rng, dims, cuts, -0.22, 0.18)
    return jnp.clip(array, -limit, limit).astype(kind)


def setup_inputs(seed: int = 0) -> dict:
    splits = jax.random.split(jax.random.key(seed), 15)
    hidden_in = gaussian(splits[0], (MB, SEQS, SEQ, D), 1.0, 6.0, ((1, 32),))
    segment_ids = jax.vmap(lambda own: jnp.searchsorted(jnp.cumsum(uneven(own, 8, SEQ, SEQ // 4, 1)), jnp.arange(SEQ), side="right"))(jax.random.split(splits[1], MB * SEQS)).reshape((MB, SEQS, SEQ)).astype(jnp.int32)
    bucket_ids = with_ends(jax.random.randint(splits[2], (2 * SEQ - 1,), 0, BUCKETS), jax.random.fold_in(splits[2], 1), 0, BUCKETS - 1).astype(jnp.int32)
    norm1_gain = jnp.clip(1.0 + 0.1 * jax.random.normal(splits[3], (D,), jnp.float32), 0.5, 1.5).astype(jnp.bfloat16)
    rel_bias = gaussian(splits[4], (BUCKETS * H,), 1.0, 4.0, ((0, 32),))
    query_weight = gaussian(splits[5], (D, D), (16 * D) ** -0.5, 0.046875, ((0, 32),))
    key_weight = gaussian(splits[6], (D, D), D ** -0.5, 0.1875, ((0, 32),))
    value_weight = gaussian(splits[7], (D, D), D ** -0.5, 0.1875, ((0, 32),))
    output_weight = gaussian(splits[8], (D, D), (D // 16) ** -0.5, 0.75, ((0, 32),))
    norm2_gain = jnp.clip(1.0 + 0.1 * jax.random.normal(splits[9], (D,), jnp.float32), 0.5, 1.5).astype(jnp.bfloat16)
    gate_weight = gaussian(splits[10], (D, FF), D ** -0.5, 0.1875, ((0, 32),))
    up_weight = gaussian(splits[11], (D, FF), D ** -0.5, 0.1875, ((0, 32),))
    down_weight = gaussian(splits[12], (FF, D), FF ** -0.5, 0.109375, ((0, 32),))
    out_grad = gaussian(splits[13], (MB, SEQS, SEQ, D), 1.0, 6.0, ((1, 32),))
    return {"hidden_in": hidden_in, "segment_ids": segment_ids, "bucket_ids": bucket_ids, "norm1_gain": norm1_gain, "rel_bias": rel_bias, "query_weight": query_weight, "key_weight": key_weight, "value_weight": value_weight, "output_weight": output_weight, "norm2_gain": norm2_gain, "gate_weight": gate_weight, "up_weight": up_weight, "down_weight": down_weight, "out_grad": out_grad}


@jax.custom_vjp
def low(v):
    return lax.optimization_barrier(v.astype(jnp.bfloat16)).astype(jnp.float32)

@jax.custom_vjp
def low_back(v):
    return v

def low_keep(v):
    return (low(v), None)

def low_pass(kept, grad):
    return (grad,)

def back_keep(v):
    return (v, None)

def back_low(kept, grad):
    return (low(grad),)
low.defvjp(low_keep, low_pass)
low_back.defvjp(back_keep, back_low)
EPSILON = 1e-06
HIGHEST = lax.Precision.HIGHEST
MASKED = -1000000000.0

def norm_apply(values, gain_vec):
    return values * lax.rsqrt(lax.optimization_barrier(jnp.mean(values * values, axis=-1, keepdims=True)) + EPSILON) * gain_vec

def position_bias(bias_table, bucket_ids):
    length = (bucket_ids.shape[0] + 1) // 2
    per_offset = bias_table.reshape(BUCKETS, H)[bucket_ids]
    places = jnp.arange(length, dtype=jnp.int32)
    offset_index = (places[None, :] - places[:, None] + (length - 1)).astype(jnp.int32)
    return jnp.transpose(per_offset[offset_index], (2, 0, 1))

def attend(pos_bias, queries, key_rows, value_rows, segments):
    q_heads = queries.reshape(-1, H, DH)
    k_heads = key_rows.reshape(-1, H, DH)
    v_heads = value_rows.reshape(-1, H, DH)
    scores = low_back(jnp.einsum('qhd,khd->hqk', q_heads, k_heads, precision=HIGHEST) + pos_bias)
    same_doc = segments[:, None] == segments[None, :]
    scores = jnp.where(same_doc[None], scores, MASKED)
    attention = low(jax.nn.softmax(scores, axis=-1))
    mixed_rows = jnp.einsum('hqk,khd->qhd', attention, v_heads, precision=HIGHEST)
    return mixed_rows.reshape(-1, H * DH)

def layer(inputs, segments, bucket_ids, params):
    gain_one, bias_table, w_query, w_key, w_value, w_output, gain_two, w_gate, w_up, w_down = params
    sequences = inputs.shape[0]
    tok_rows = inputs.reshape(-1, D)
    normed = low(norm_apply(tok_rows, gain_one))
    queries = low(low_back(jnp.dot(normed, w_query, precision=HIGHEST)))
    key_rows = low(low_back(jnp.dot(normed, w_key, precision=HIGHEST)))
    value_rows = low(low_back(jnp.dot(normed, w_value, precision=HIGHEST)))
    pos_bias = position_bias(bias_table, bucket_ids)
    checked = jax.checkpoint(attend)
    mixed_rows = lax.map(lambda pieces: checked(pos_bias, pieces[0], pieces[1], pieces[2], pieces[3]), (queries.reshape(sequences, SEQ, D), key_rows.reshape(sequences, SEQ, D), value_rows.reshape(sequences, SEQ, D), segments))
    mixed_rows = low(low_back(mixed_rows.reshape(-1, D)))
    residual = tok_rows + low_back(jnp.dot(mixed_rows, w_output, precision=HIGHEST))
    second = low(norm_apply(residual, gain_two))
    gate_value = low_back(jnp.dot(second, w_gate, precision=HIGHEST))
    up_part = low_back(jnp.dot(second, w_up, precision=HIGHEST))
    hidden = low(jax.nn.gelu(gate_value, approximate=True) * up_part)
    result = residual + low_back(jnp.dot(hidden, w_down, precision=HIGHEST))
    return result.reshape(inputs.shape)

def reference(hidden_in, segment_ids, bucket_ids, norm1_gain, rel_bias, query_weight, key_weight, value_weight, output_weight, norm2_gain, gate_weight, up_weight, down_weight, out_grad):
    params = tuple((weight.astype(jnp.float32) for weight in (norm1_gain, rel_bias, query_weight, key_weight, value_weight, output_weight, norm2_gain, gate_weight, up_weight, down_weight)))
    sequences = MB * SEQS
    group = math.gcd(sequences, max(1, 4096 // SEQ))
    inputs = hidden_in.reshape(sequences // group, group, SEQ, D)
    segments = segment_ids.reshape(sequences // group, group, SEQ)
    cotangents = out_grad.reshape(sequences // group, group, SEQ, D)

    def advance(totals, pieces):
        inputs_now, segments_now, cotangent = pieces
        outputs, pullback = jax.vjp(lambda values, weights: layer(values, segments_now, bucket_ids, weights), inputs_now.astype(jnp.float32), params)
        input_part, weight_grads = pullback(cotangent.astype(jnp.float32))
        totals = tuple((total + grad_now for total, grad_now in zip(totals, weight_grads)))
        return (totals, (outputs.astype(jnp.bfloat16), input_part.astype(jnp.bfloat16)))
    zeros = tuple((jnp.zeros(weight.shape, jnp.float32) for weight in params))
    totals, (outputs, input_parts) = lax.scan(advance, zeros, (inputs, segments, cotangents))
    return (outputs.reshape(hidden_in.shape), input_parts.reshape(hidden_in.shape), totals[0], totals[1], totals[2], totals[3], totals[4], totals[5], totals[6], totals[7], totals[8], totals[9])
```

```python
import functools

import jax
import jax.numpy as jnp
from jax import lax
from jax.experimental import pallas as pl
from jax.experimental.pallas import tpu as pltpu
from jax.sharding import PartitionSpec as P

H = 16
DH = 64
BUCKETS = 32
AXES = ("wide", "narrow")
EPSILON = 1e-06
HIGHEST = lax.Precision.HIGHEST
MASKED = -1000000000.0
F32 = jnp.float32
BF16 = jnp.bfloat16
TILE = 128


def halve_order(count, first):
    bits = count.bit_length() - 1
    return [b for b in first if b < bits] + [b for b in range(bits) if b not in first]


def my_bit(bit):
    return (lax.axis_index(AXES) >> bit) & 1


def pairs(bit, count):
    return [(i, i ^ (1 << bit)) for i in range(count)]


def sum_to_owner(parts, count, order):
    bits = count.bit_length() - 1
    rest = parts.shape[1:]
    parts = parts.reshape((2,) * bits + rest)
    dims = list(range(bits - 1, -1, -1))
    wide_sum = parts.dtype == F32
    for step, bit in enumerate(order):
        axis, mine = dims.index(bit), my_bit(bit)
        keep = lax.dynamic_index_in_dim(parts, mine, axis, keepdims=False)
        send = lax.dynamic_index_in_dim(parts, 1 - mine, axis, keepdims=False)
        got = lax.ppermute(send, AXES, pairs(bit, count))
        total = keep.astype(F32) + got.astype(F32)
        parts = total if wide_sum or step == len(order) - 1 else total.astype(BF16)
        dims.pop(axis)
    return parts


def gather(block):
    return lax.all_gather(block, AXES, axis=0, tiled=True)


def windows(length):
    out = []
    for start in range(0, length, TILE):
        low, high = max(0, start - TILE), min(length, start + 2 * TILE)
        out.append((start, low, high - low, low - start + TILE))
    return out


def head_mask(head, dtype):
    lane = lax.broadcasted_iota(jnp.int32, (1, 2 * DH), 1)
    return ((lane // DH) == head).astype(dtype)


NT = (((1,), (1,)), ((), ()))
TN = (((0,), (0,)), ((), ()))


def block_probs(query, key, bias, seg_q, seg_k):
    scores = lax.dot_general(query, key, NT, preferred_element_type=F32) + bias
    scores = jnp.where(seg_q == seg_k, scores, MASKED)
    expo = jnp.exp(scores - jnp.max(scores, axis=-1, keepdims=True))
    return expo / jnp.sum(expo, axis=-1, keepdims=True)


def attend_kernel(q_ref, k_ref, v_ref, bias_ref, col_ref, row_ref, out_ref):
    for start, low, keys, left in windows(q_ref.shape[0]):
        query = q_ref[pl.ds(start, TILE), :]
        key = k_ref[pl.ds(low, keys), :]
        value = v_ref[pl.ds(low, keys), :]
        seg_q = col_ref[0, pl.ds(start, TILE), :]
        seg_k = row_ref[0, :, pl.ds(low, keys)]
        mixed = jnp.zeros((TILE, 2 * DH), F32)
        for head in range(2):
            mask = head_mask(head, BF16)
            probs = block_probs(
                query * mask, key, bias_ref[head, :, pl.ds(left, keys)], seg_q, seg_k
            )
            mixed += jnp.dot(probs.astype(BF16), value * mask, preferred_element_type=F32)
        out_ref[pl.ds(start, TILE), :] = mixed.astype(BF16)


def attend_back_kernel(
    q_ref, k_ref, v_ref, dm_ref, bias_ref, col_ref, row_ref,
    dq_ref, dk_ref, dv_ref, dbias_ref, dk_sum, dv_sum,
):
    @pl.when(pl.program_id(1) == 0)
    def _():
        dbias_ref[...] = jnp.zeros_like(dbias_ref)

    dk_sum[...] = jnp.zeros_like(dk_sum)
    dv_sum[...] = jnp.zeros_like(dv_sum)
    for start, low, keys, left in windows(q_ref.shape[0]):
        query = q_ref[pl.ds(start, TILE), :]
        grad = dm_ref[pl.ds(start, TILE), :]
        key = k_ref[pl.ds(low, keys), :]
        value = v_ref[pl.ds(low, keys), :]
        seg_q = col_ref[0, pl.ds(start, TILE), :]
        seg_k = row_ref[0, :, pl.ds(low, keys)]
        dq = jnp.zeros((TILE, 2 * DH), F32)
        for head in range(2):
            mask = head_mask(head, BF16)
            q_h, g_h = query * mask, grad * mask
            probs = block_probs(q_h, key, bias_ref[head, :, pl.ds(left, keys)], seg_q, seg_k)
            dprob = lax.dot_general(g_h, value, NT, preferred_element_type=F32)
            centre = jnp.sum(probs * dprob, axis=-1, keepdims=True)
            dscore = (probs * (dprob - centre)).astype(BF16)
            dbias_ref[head, :, pl.ds(left, keys)] += dscore.astype(F32)
            dq += jnp.dot(dscore, key * mask, preferred_element_type=F32)
            dk_sum[pl.ds(low, keys), :] += lax.dot_general(
                dscore, q_h, TN, preferred_element_type=F32
            )
            dv_sum[pl.ds(low, keys), :] += lax.dot_general(
                probs.astype(BF16), g_h, TN, preferred_element_type=F32
            )
        dq_ref[pl.ds(start, TILE), :] = dq.astype(BF16)
    dk_ref[...] = dk_sum[...].astype(BF16)
    dv_ref[...] = dv_sum[...].astype(BF16)


def attend_specs(length):
    def lanes(offset):
        return pl.BlockSpec((length, 2 * DH), lambda pair, seq: (seq, pair + offset))

    bias = pl.BlockSpec((2, TILE, 3 * TILE), lambda pair, seq: (pair, 0, 0))
    col = pl.BlockSpec((1, length, 1), lambda pair, seq: (seq, 0, 0))
    row = pl.BlockSpec((1, 1, length), lambda pair, seq: (seq, 0, 0))
    return lanes, bias, col, row


def attend(qkv, bias_tiles, segments):
    sequences, length = segments.shape
    lanes, bias, col, row = attend_specs(length)
    width = H * DH
    steps = width // (2 * DH)
    work = sequences * H * length * 3 * TILE
    return pl.pallas_call(
        attend_kernel,
        grid=(steps, sequences),
        in_specs=[lanes(0), lanes(steps), lanes(2 * steps), bias, col, row],
        out_specs=lanes(0),
        out_shape=jax.ShapeDtypeStruct((sequences * length, width), BF16),
        name="attend",
        cost_estimate=pl.CostEstimate(
            flops=4 * work * 2 * DH, transcendentals=work, bytes_accessed=8 * qkv.size // 3
        ),
    )(qkv, qkv, qkv, bias_tiles, segments[:, :, None], segments[:, None, :])


def attend_back(qkv, mixed_grad, bias_tiles, segments):
    sequences, length = segments.shape
    lanes, bias, col, row = attend_specs(length)
    width = H * DH
    steps = width // (2 * DH)
    rows = sequences * length
    work = sequences * H * length * 3 * TILE
    flat = jax.ShapeDtypeStruct((rows, width), BF16)
    return pl.pallas_call(
        attend_back_kernel,
        grid=(steps, sequences),
        in_specs=[lanes(0), lanes(steps), lanes(2 * steps), lanes(0), bias, col, row],
        out_specs=[lanes(0), lanes(0), lanes(0), bias],
        out_shape=[flat, flat, flat, jax.ShapeDtypeStruct((H, TILE, 3 * TILE), F32)],
        scratch_shapes=[pltpu.VMEM((length, 2 * DH), F32), pltpu.VMEM((length, 2 * DH), F32)],
        name="attend_back",
        cost_estimate=pl.CostEstimate(
            flops=10 * work * 2 * DH, transcendentals=work, bytes_accessed=14 * qkv.size // 3
        ),
    )(qkv, qkv, qkv, mixed_grad, bias_tiles, segments[:, :, None], segments[:, None, :])


def near_buckets(bucket_ids):
    centre = (bucket_ids.shape[0] + 1) // 2 - 1
    near = bucket_ids[centre - (2 * TILE - 1) : centre + 2 * TILE]
    return (near[:, None] == jnp.arange(BUCKETS, dtype=jnp.int32)[None, :]).astype(F32)


def bias_tiles_of(table, bucket_ids):
    chosen = near_buckets(bucket_ids)
    offsets = jnp.dot(chosen, table.reshape(BUCKETS, H), precision=HIGHEST).T
    span = offsets.shape[1] + 1
    padded = jnp.pad(offsets, ((0, 0), (0, 1)))
    rows = jnp.broadcast_to(padded[:, None, :], (H, TILE, span)).reshape(H, -1)
    rows = rows[:, : TILE * (span - 1)].reshape(H, TILE, span - 1)
    return rows[:, :, TILE - 1 : TILE - 1 + 3 * TILE]


def table_grad_of(tile_sums, bucket_ids):
    chosen = near_buckets(bucket_ids)
    span = 4 * TILE
    rows = jnp.pad(tile_sums, ((0, 0), (0, 0), (TILE - 1, 0)))
    rows = jnp.pad(rows.reshape(H, -1), ((0, 0), (0, TILE))).reshape(H, TILE, span)
    offsets = jnp.sum(rows, axis=1)[:, : span - 1]
    return jnp.dot(chosen.T, offsets.T, precision=HIGHEST).reshape(-1)


def dot(left, right):
    return jnp.dot(left, right, preferred_element_type=F32)


def dot_nt(left, right):
    return lax.dot_general(left, right, NT, preferred_element_type=F32)


def dot_tn(left, right):
    return lax.dot_general(left, right, TN, preferred_element_type=F32)


def scale_of(rows):
    return lax.rsqrt(jnp.mean(rows * rows, axis=-1, keepdims=True) + EPSILON)


def norm_back(rows, scale, gain, upstream):
    weighted = upstream * gain
    inner = jnp.mean(rows * weighted, axis=-1, keepdims=True)
    rows_grad = scale * weighted - rows * (scale * scale * scale) * inner
    gain_grad = jnp.sum(rows * scale * upstream, axis=0)
    return rows_grad, gain_grad


def gated(gate_value, up_part):
    return jax.nn.gelu(gate_value, approximate=True) * up_part


def body(
    hidden_in, segment_ids, bucket_ids, norm1_gain, rel_bias, query_weight, key_weight,
    value_weight, output_weight, norm2_gain, gate_weight, up_weight, down_weight, out_grad,
):
    count = lax.axis_size("wide") * lax.axis_size("narrow")
    length, width = hidden_in.shape[2:]
    inner = gate_weight.shape[1]
    own, own_bias = norm1_gain.shape[0], rel_bias.shape[0]
    own_inner = down_weight.shape[0]

    small = jnp.zeros((own, 128), BF16)
    small = small.at[0, :own].set(norm1_gain).at[1, :own].set(norm2_gain)
    small = small.at[2, :own_bias].set(rel_bias)
    first = gather(jnp.concatenate([query_weight, key_weight, value_weight, small], axis=1))
    later = gather(jnp.concatenate([output_weight, gate_weight, up_weight], axis=1))
    w_down = gather(down_weight)
    w_qkv = first[:, : 3 * width]
    smalls = first[:, 3 * width :].reshape(count, own, 128)
    gain_one = smalls[:, 0, :own].reshape(-1).astype(F32)
    gain_two = smalls[:, 1, :own].reshape(-1).astype(F32)
    table = smalls[:, 2, :own_bias].reshape(-1).astype(F32)
    w_output = later[:, :width]
    w_gate = later[:, width : width + inner]
    w_up = later[:, width + inner :]

    segments = segment_ids.reshape(-1, length)
    rows = hidden_in.reshape(-1, width).astype(F32)
    out_rows = out_grad.reshape(-1, width)

    scale_one = scale_of(rows)
    normed = (rows * scale_one * gain_one).astype(BF16)
    qkv = dot(normed, w_qkv).astype(BF16)
    bias_tiles = bias_tiles_of(table, bucket_ids)
    mixed = attend(qkv, bias_tiles, segments)
    residual = rows + dot(mixed, w_output)
    scale_two = scale_of(residual)
    second = (residual * scale_two * gain_two).astype(BF16)
    gate_value = dot(second, w_gate)
    up_part = dot(second, w_up)
    hidden = gated(gate_value, up_part).astype(BF16)

    def scatter(grad, order):
        return sum_to_owner(grad.reshape(count, -1, grad.shape[-1]), count, halve_order(count, order))

    down_grad = scatter(dot_tn(hidden, out_rows).astype(BF16), (2, 1, 3, 4, 0))
    result = (residual + dot(hidden, w_down)).astype(BF16)

    hidden_grad = dot_nt(out_rows, w_down)
    _, pull_gate = jax.vjp(gated, gate_value, up_part)
    gate_grad, up_grad = pull_gate(hidden_grad)
    gate_grad, up_grad = gate_grad.astype(BF16), up_grad.astype(BF16)
    gate_weight_grad = scatter(dot_tn(second, gate_grad).astype(BF16), (2, 0, 1, 3, 4))
    up_weight_grad = scatter(dot_tn(second, up_grad).astype(BF16), (2, 0, 3, 1, 4))
    second_grad = dot_nt(gate_grad, w_gate) + dot_nt(up_grad, w_up)
    residual_part, gain_two_grad = norm_back(residual, scale_two, gain_two, second_grad)
    residual_grad = out_rows.astype(F32) + residual_part
    branch_grad = residual_grad.astype(BF16)
    mixed_grad = dot_nt(branch_grad, w_output).astype(BF16)
    output_weight_grad = scatter(dot_tn(mixed, branch_grad).astype(BF16), (2, 1, 0, 3, 4))

    dq, dk, dv, tile_sums = attend_back(qkv, mixed_grad, bias_tiles, segments)
    value_weight_grad = scatter(dot_tn(normed, dv).astype(BF16), (2, 0, 1, 3, 4))
    key_weight_grad = scatter(dot_tn(normed, dk).astype(BF16), (2, 1, 0, 3, 4))
    query_weight_grad = scatter(dot_tn(normed, dq).astype(BF16), (2, 0, 1, 3, 4))
    normed_grad = (
        dot_nt(dq, w_qkv[:, :width])
        + dot_nt(dk, w_qkv[:, width : 2 * width])
        + dot_nt(dv, w_qkv[:, 2 * width :])
    )
    rows_part, gain_one_grad = norm_back(rows, scale_one, gain_one, normed_grad)
    input_grad = (residual_grad + rows_part).astype(BF16)
    table_grad = table_grad_of(tile_sums, bucket_ids)

    def wide_rows(vector):
        return jnp.pad(vector.reshape(count, 1, -1), ((0, 0), (0, 0), (0, 128 - vector.size // count)))

    tiny = jnp.concatenate(
        [wide_rows(gain_one_grad), wide_rows(gain_two_grad), wide_rows(table_grad)], axis=1
    )
    tiny = sum_to_owner(jnp.pad(tiny, ((0, 0), (0, 5), (0, 0))), count, halve_order(count, (2, 0, 1)))
    return (
        result.reshape(hidden_in.shape),
        input_grad.reshape(hidden_in.shape),
        tiny[0, :own],
        tiny[2, :own_bias],
        query_weight_grad,
        key_weight_grad,
        value_weight_grad,
        output_weight_grad,
        tiny[1, :own],
        gate_weight_grad,
        up_weight_grad,
        down_grad,
    )


def solution(mesh):
    split, rows, tokens = P(AXES), P(AXES, None), P(None, AXES, None, None)
    in_specs = (
        tokens, P(None, AXES, None), P(), split, split, rows, rows, rows, rows,
        split, rows, rows, rows, tokens,
    )
    out_specs = (tokens, tokens, split, split, rows, rows, rows, rows, split, rows, rows, rows)
    return jax.shard_map(body, mesh=mesh, in_specs=in_specs, out_specs=out_specs, check_vma=False)
```

```python
import functools

import jax
import jax.numpy as jnp
from jax import lax
from jax.experimental import pallas as pl
from jax.experimental.pallas import tpu as pltpu
from jax.sharding import PartitionSpec as P

H = 16
DH = 64
BUCKETS = 32
AXES = ("wide", "narrow")
EPSILON = 1e-06
HIGHEST = lax.Precision.HIGHEST
MASKED = -1000000000.0
F32 = jnp.float32
BF16 = jnp.bfloat16
TILE = 128


def halve_order(count, first):
    bits = count.bit_length() - 1
    return [b for b in first if b < bits] + [b for b in range(bits) if b not in first]


def my_bit(bit):
    return (lax.axis_index(AXES) >> bit) & 1


def pairs(bit, count):
    return [(i, i ^ (1 << bit)) for i in range(count)]


class Sums:
    def __init__(self, grad, count, order):
        bits = count.bit_length() - 1
        self.count, self.order = count, halve_order(count, order)
        self.dims = list(range(bits - 1, -1, -1))
        self.exact = grad.dtype == F32
        self.parts = grad.reshape((2,) * bits + (-1, grad.shape[-1]))
        self.flying = None
        self.start()

    def start(self):
        bit = self.order.pop(0)
        axis, mine = self.dims.index(bit), my_bit(bit)
        self.dims.pop(axis)
        keep = lax.dynamic_index_in_dim(self.parts, mine, axis, keepdims=False)
        send = lax.dynamic_index_in_dim(self.parts, 1 - mine, axis, keepdims=False)
        self.flying = [keep, lax.ppermute(send, AXES, pairs(bit, self.count))]

    def step(self):
        total = self.flying[0].astype(F32) + self.flying[1].astype(F32)
        self.parts = total if self.exact or not self.order else total.astype(BF16)
        self.flying = None
        if self.order:
            self.start()

    def finish(self):
        while self.flying is not None:
            self.step()
        return self.parts


def meet(value, *sums):
    sums = [one for one in sums if one.flying is not None]
    value, got = lax.optimization_barrier((value, [one.flying[1] for one in sums]))
    for one, arrived in zip(sums, got):
        one.flying[1] = arrived
        one.step()
    return value


def gather(block):
    return lax.all_gather(block, AXES, axis=0, tiled=True)


def windows(length):
    out = []
    for start in range(0, length, TILE):
        low, high = max(0, start - TILE), min(length, start + 2 * TILE)
        out.append((start, low, high - low, low - start + TILE))
    return out


NT = (((1,), (1,)), ((), ()))
TN = (((0,), (0,)), ((), ()))


def by_head(rows):
    first = lax.broadcasted_iota(jnp.int32, (1, 2 * DH), 1) < DH
    zero = jnp.zeros_like(rows)
    return jnp.concatenate([jnp.where(first, rows, zero), jnp.where(first, zero, rows)], axis=0)


def join_heads(stacked):
    first = lax.broadcasted_iota(jnp.int32, (1, 2 * DH), 1) < DH
    return jnp.where(first, stacked[:TILE], stacked[TILE:])


def spread_bias(offsets_ref, tile_ref):
    for head in range(2):
        rows = jnp.broadcast_to(offsets_ref[head], (TILE, 4 * TILE))
        rolled = pltpu.roll(rows, 3 * TILE + 1, 1, stride=1, stride_axis=0)
        tile_ref[pl.ds(head * TILE, TILE), :] = rolled[:, : 3 * TILE]


def block_probs(query, key, bias, seg_q, seg_k):
    scores = lax.dot_general(query, key, NT, preferred_element_type=F32) + bias
    scores = jnp.where(seg_q == seg_k, scores, MASKED)
    expo = jnp.exp(scores - jnp.max(scores, axis=-1, keepdims=True))
    return expo * (1.0 / jnp.sum(expo, axis=-1, keepdims=True))


def attend_kernel(q_ref, k_ref, v_ref, offsets_ref, col_ref, row_ref, out_ref, tile_ref):
    @pl.when(pl.program_id(1) == 0)
    def _():
        spread_bias(offsets_ref, tile_ref)

    for start, low, keys, left in windows(q_ref.shape[0]):
        seg_q = col_ref[0, pl.ds(start, TILE), :]
        probs = block_probs(
            by_head(q_ref[pl.ds(start, TILE), :]),
            k_ref[pl.ds(low, keys), :],
            tile_ref[:, pl.ds(left, keys)],
            jnp.concatenate([seg_q, seg_q], axis=0),
            row_ref[0, :, pl.ds(low, keys)],
        )
        mixed = jnp.dot(
            probs.astype(BF16), v_ref[pl.ds(low, keys), :], preferred_element_type=F32
        )
        out_ref[pl.ds(start, TILE), :] = join_heads(mixed).astype(BF16)


def attend_back_kernel(
    q_ref, k_ref, v_ref, dm_ref, offsets_ref, col_ref, row_ref,
    dq_ref, dk_ref, dv_ref, dbias_ref, dk_sum, dv_sum, tile_ref,
):
    @pl.when(pl.program_id(1) == 0)
    def _():
        spread_bias(offsets_ref, tile_ref)
        dbias_ref[...] = jnp.zeros_like(dbias_ref)

    dk_sum[...] = jnp.zeros_like(dk_sum)
    dv_sum[...] = jnp.zeros_like(dv_sum)
    for start, low, keys, left in windows(q_ref.shape[0]):
        query = by_head(q_ref[pl.ds(start, TILE), :])
        grad = by_head(dm_ref[pl.ds(start, TILE), :])
        key = k_ref[pl.ds(low, keys), :]
        value = v_ref[pl.ds(low, keys), :]
        seg_q = col_ref[0, pl.ds(start, TILE), :]
        probs = block_probs(
            query, key, tile_ref[:, pl.ds(left, keys)],
            jnp.concatenate([seg_q, seg_q], axis=0), row_ref[0, :, pl.ds(low, keys)],
        )
        dprob = lax.dot_general(grad, value, NT, preferred_element_type=F32)
        centre = jnp.sum(probs * dprob, axis=-1, keepdims=True)
        dscore = (probs * (dprob - centre)).astype(BF16)
        wide = dscore.astype(F32)
        dbias_ref[0, :, pl.ds(left, keys)] += wide[:TILE]
        dbias_ref[1, :, pl.ds(left, keys)] += wide[TILE:]
        dq = jnp.dot(dscore, key, preferred_element_type=F32)
        dq_ref[pl.ds(start, TILE), :] = join_heads(dq).astype(BF16)
        dk_sum[pl.ds(low, keys), :] += lax.dot_general(
            dscore, query, TN, preferred_element_type=F32
        )
        dv_sum[pl.ds(low, keys), :] += lax.dot_general(
            probs.astype(BF16), grad, TN, preferred_element_type=F32
        )
    dk_ref[...] = dk_sum[...].astype(BF16)
    dv_ref[...] = dv_sum[...].astype(BF16)


def attend_specs(length):
    def lanes(offset):
        return pl.BlockSpec((length, 2 * DH), lambda pair, seq: (seq, pair + offset))

    bias = pl.BlockSpec((2, 1, 4 * TILE), lambda pair, seq: (pair, 0, 0))
    col = pl.BlockSpec((1, length, 1), lambda pair, seq: (seq, 0, 0))
    row = pl.BlockSpec((1, 1, length), lambda pair, seq: (seq, 0, 0))
    return lanes, bias, col, row


def attend(qkv, offsets, segments):
    sequences, length = segments.shape
    lanes, bias, col, row = attend_specs(length)
    width = H * DH
    steps = width // (2 * DH)
    work = sequences * H * length * 3 * TILE
    return pl.pallas_call(
        attend_kernel,
        grid=(steps, sequences),
        in_specs=[lanes(0), lanes(steps), lanes(2 * steps), bias, col, row],
        out_specs=lanes(0),
        out_shape=jax.ShapeDtypeStruct((sequences * length, width), BF16),
        scratch_shapes=[pltpu.VMEM((2 * TILE, 3 * TILE), F32)],
        name="attend",
        cost_estimate=pl.CostEstimate(
            flops=4 * work * 2 * DH, transcendentals=work, bytes_accessed=8 * qkv.size // 3
        ),
    )(qkv, qkv, qkv, offsets, segments[:, :, None], segments[:, None, :])


def attend_back(qkv, mixed_grad, offsets, segments):
    sequences, length = segments.shape
    lanes, bias, col, row = attend_specs(length)
    width = H * DH
    steps = width // (2 * DH)
    rows = sequences * length
    work = sequences * H * length * 3 * TILE
    flat = jax.ShapeDtypeStruct((rows, width), BF16)
    return pl.pallas_call(
        attend_back_kernel,
        grid=(steps, sequences),
        in_specs=[lanes(0), lanes(steps), lanes(2 * steps), lanes(0), bias, col, row],
        out_specs=[
            lanes(0), lanes(0), lanes(0),
            pl.BlockSpec((2, TILE, 3 * TILE), lambda pair, seq: (pair, 0, 0)),
        ],
        out_shape=[flat, flat, flat, jax.ShapeDtypeStruct((H, TILE, 3 * TILE), F32)],
        scratch_shapes=[
            pltpu.VMEM((length, 2 * DH), F32),
            pltpu.VMEM((length, 2 * DH), F32),
            pltpu.VMEM((2 * TILE, 3 * TILE), F32),
        ],
        name="attend_back",
        cost_estimate=pl.CostEstimate(
            flops=10 * work * 2 * DH, transcendentals=work, bytes_accessed=14 * qkv.size // 3
        ),
    )(qkv, qkv, qkv, mixed_grad, offsets, segments[:, :, None], segments[:, None, :])


def near_buckets(bucket_ids):
    centre = (bucket_ids.shape[0] + 1) // 2 - 1
    near = bucket_ids[centre - (2 * TILE - 1) : centre + 2 * TILE]
    return (near[:, None] == jnp.arange(BUCKETS, dtype=jnp.int32)[None, :]).astype(F32)


def offsets_of(table, bucket_ids):
    chosen = near_buckets(bucket_ids)
    offsets = jnp.dot(chosen, table.reshape(BUCKETS, H), precision=HIGHEST).T
    return jnp.pad(offsets, ((0, 0), (0, 1)))[:, None, :]


def table_grad_of(tile_sums, bucket_ids):
    chosen = near_buckets(bucket_ids)
    span = 4 * TILE
    rows = jnp.pad(tile_sums, ((0, 0), (0, 0), (TILE - 1, 0)))
    rows = jnp.pad(rows.reshape(H, -1), ((0, 0), (0, TILE))).reshape(H, TILE, span)
    offsets = jnp.sum(rows, axis=1)[:, : span - 1]
    return jnp.dot(chosen.T, offsets.T, precision=HIGHEST).reshape(-1)


def dot(left, right):
    return jnp.dot(left, right, preferred_element_type=F32)


def dot_nt(left, right):
    return lax.dot_general(left, right, NT, preferred_element_type=F32)


def dot_tn(left, right):
    return lax.dot_general(left, right, TN, preferred_element_type=F32)


def scale_of(rows):
    return lax.rsqrt(jnp.mean(rows * rows, axis=-1, keepdims=True) + EPSILON)


def norm_back(rows, scale, gain, upstream):
    weighted = upstream * gain
    inner = jnp.mean(rows * weighted, axis=-1, keepdims=True)
    rows_grad = scale * weighted - rows * (scale * scale * scale) * inner
    gain_grad = jnp.sum(rows * scale * upstream, axis=0)
    return rows_grad, gain_grad


def gated(gate_value, up_part):
    return jax.nn.gelu(gate_value, approximate=True) * up_part


def body(
    hidden_in, segment_ids, bucket_ids, norm1_gain, rel_bias, query_weight, key_weight,
    value_weight, output_weight, norm2_gain, gate_weight, up_weight, down_weight, out_grad,
):
    count = lax.axis_size("wide") * lax.axis_size("narrow")
    length, width = hidden_in.shape[2:]
    inner = gate_weight.shape[1]
    own, own_bias = norm1_gain.shape[0], rel_bias.shape[0]
    own_inner = down_weight.shape[0]

    small = jnp.zeros((own, 128), BF16)
    small = small.at[0, :own].set(norm1_gain).at[1, :own].set(norm2_gain)
    small = small.at[2, :own_bias].set(rel_bias)
    first = gather(jnp.concatenate([query_weight, key_weight, value_weight, small], axis=1))
    later = jnp.concatenate([output_weight, gate_weight, up_weight], axis=1)
    first, later = lax.optimization_barrier((first, later))
    later = gather(later)
    later, down_weight = lax.optimization_barrier((later, down_weight))
    w_down = gather(down_weight)
    w_qkv = first[:, : 3 * width]
    smalls = first[:, 3 * width :].reshape(count, own, 128)
    gain_one = smalls[:, 0, :own].reshape(-1).astype(F32)
    gain_two = smalls[:, 1, :own].reshape(-1).astype(F32)
    table = smalls[:, 2, :own_bias].reshape(-1).astype(F32)
    w_output = later[:, :width]
    w_gate = later[:, width : width + inner]
    w_up = later[:, width + inner :]

    segments = segment_ids.reshape(-1, length)
    rows = hidden_in.reshape(-1, width).astype(F32)
    out_rows = out_grad.reshape(-1, width)

    scale_one = scale_of(rows)
    normed = (rows * scale_one * gain_one).astype(BF16)
    qkv = dot(normed, w_qkv).astype(BF16)
    offsets = offsets_of(table, bucket_ids)
    mixed = attend(qkv, offsets, segments)
    residual = rows + dot(mixed, w_output)
    scale_two = scale_of(residual)
    second = (residual * scale_two * gain_two).astype(BF16)
    gate_value = dot(second, w_gate)
    up_part = dot(second, w_up)
    hidden = gated(gate_value, up_part).astype(BF16)

    def scatter(grad, order):
        return Sums(grad.astype(BF16), count, order)

    down_sum = scatter(dot_tn(hidden, out_rows), (2, 1, 3, 4, 0))
    hidden_grad = dot_nt(out_rows, w_down)
    _, pull_gate = jax.vjp(gated, gate_value, up_part)
    gate_grad, up_grad = pull_gate(hidden_grad)
    gate_grad, up_grad = gate_grad.astype(BF16), up_grad.astype(BF16)
    gate_grad = meet(gate_grad, down_sum)
    gate_sum = scatter(dot_tn(second, gate_grad), (2, 0, 1, 3, 4))
    up_sum = scatter(dot_tn(second, up_grad), (2, 0, 3, 1, 4))
    second_grad = dot_nt(gate_grad, w_gate) + dot_nt(up_grad, w_up)
    residual_part, gain_two_grad = norm_back(residual, scale_two, gain_two, second_grad)
    residual_grad = out_rows.astype(F32) + residual_part
    branch_grad = residual_grad.astype(BF16)
    branch_grad = meet(branch_grad, down_sum, gate_sum, up_sum)
    mixed_grad = dot_nt(branch_grad, w_output).astype(BF16)
    output_sum = scatter(dot_tn(mixed, branch_grad), (2, 1, 0, 3, 4))
    result = (residual + dot(hidden, w_down)).astype(BF16)
    mixed_grad, result = lax.optimization_barrier((mixed_grad, result))

    dq, dk, dv, tile_sums = attend_back(qkv, mixed_grad, offsets, segments)
    dv = meet(dv, down_sum, gate_sum, up_sum, output_sum)
    value_sum = scatter(dot_tn(normed, dv), (2, 0, 1, 3, 4))
    key_sum = scatter(dot_tn(normed, dk), (2, 1, 0, 3, 4))
    query_sum = scatter(dot_tn(normed, dq), (2, 0, 1, 3, 4))
    dq = meet(dq, down_sum, gate_sum, up_sum, output_sum)
    normed_grad = (
        dot_nt(dq, w_qkv[:, :width])
        + dot_nt(dk, w_qkv[:, width : 2 * width])
        + dot_nt(dv, w_qkv[:, 2 * width :])
    )
    rows_part, gain_one_grad = norm_back(rows, scale_one, gain_one, normed_grad)
    input_grad = (residual_grad + rows_part).astype(BF16)
    table_grad = table_grad_of(tile_sums, bucket_ids)

    def wide_rows(vector):
        return jnp.pad(vector.reshape(count, 1, -1), ((0, 0), (0, 0), (0, 128 - vector.size // count)))

    tiny = jnp.concatenate(
        [wide_rows(gain_one_grad), wide_rows(gain_two_grad), wide_rows(table_grad)], axis=1
    )
    tiny = jnp.pad(tiny, ((0, 0), (0, 5), (0, 0))).reshape(-1, 128)
    tiny = Sums(tiny, count, (2, 0, 1)).finish()
    return (
        result.reshape(hidden_in.shape),
        input_grad.reshape(hidden_in.shape),
        tiny[0, :own],
        tiny[2, :own_bias],
        query_sum.finish(),
        key_sum.finish(),
        value_sum.finish(),
        output_sum.finish(),
        tiny[1, :own],
        gate_sum.finish(),
        up_sum.finish(),
        down_sum.finish(),
    )


def solution(mesh):
    split, rows, tokens = P(AXES), P(AXES, None), P(None, AXES, None, None)
    in_specs = (
        tokens, P(None, AXES, None), P(), split, split, rows, rows, rows, rows,
        split, rows, rows, rows, tokens,
    )
    out_specs = (tokens, tokens, split, split, rows, rows, rows, rows, split, rows, rows, rows)
    return jax.shard_map(body, mesh=mesh, in_specs=in_specs, out_specs=out_specs, check_vma=False)
```

```python
import functools

import jax
import jax.numpy as jnp
from jax import lax
from jax.experimental import pallas as pl
from jax.experimental.pallas import tpu as pltpu
from jax.sharding import PartitionSpec as P

H = 16
DH = 64
BUCKETS = 32
AXES = ("wide", "narrow")
EPSILON = 1e-06
HIGHEST = lax.Precision.HIGHEST
MASKED = -1000000000.0
F32 = jnp.float32
BF16 = jnp.bfloat16
TILE = 128


def halve_order(count, first):
    bits = count.bit_length() - 1
    return [b for b in first if b < bits] + [b for b in range(bits) if b not in first]


def my_bit(bit):
    return (lax.axis_index(AXES) >> bit) & 1


def pairs(bit, count):
    return [(i, i ^ (1 << bit)) for i in range(count)]


class Sums:
    def __init__(self, grads, count, order):
        bits = count.bit_length() - 1
        self.count, self.order = count, halve_order(count, order)
        self.dims = list(range(bits - 1, -1, -1))
        self.exact = grads[0].dtype == F32
        self.parts = [grad.reshape((2,) * bits + (-1, grad.shape[-1])) for grad in grads]
        self.flying = None
        self.start()

    def half(self, axis, index):
        halves = [
            lax.dynamic_index_in_dim(part, index, axis, keepdims=False) for part in self.parts
        ]
        return halves[0] if len(halves) == 1 else jnp.concatenate(halves, axis=-1)

    def start(self):
        bit = self.order.pop(0)
        axis, mine = self.dims.index(bit), my_bit(bit)
        self.dims.pop(axis)
        keep, send = self.half(axis, mine), self.half(axis, 1 - mine)
        self.flying = [keep, lax.ppermute(send, AXES, pairs(bit, self.count))]

    def step(self):
        total = self.flying[0].astype(F32) + self.flying[1].astype(F32)
        self.parts = [total if self.exact or not self.order else total.astype(BF16)]
        self.flying = None
        if self.order:
            self.start()

    def finish(self):
        while self.flying is not None:
            self.step()
        return self.parts[0]


def meet(value, *sums):
    sums = [one for one in sums if one.flying is not None]
    value, got = lax.optimization_barrier((value, [one.flying[1] for one in sums]))
    for one, arrived in zip(sums, got):
        one.flying[1] = arrived
        one.step()
    return value


def gather(block):
    return lax.all_gather(block, AXES, axis=0, tiled=True)


def windows(length):
    out = []
    for start in range(0, length, TILE):
        low, high = max(0, start - TILE), min(length, start + 2 * TILE)
        out.append((start, low, high - low, low - start + TILE))
    return out


NT = (((1,), (1,)), ((), ()))
TN = (((0,), (0,)), ((), ()))


def by_head(rows):
    first = lax.broadcasted_iota(jnp.int32, (1, 2 * DH), 1) < DH
    zero = jnp.zeros_like(rows)
    return jnp.concatenate([jnp.where(first, rows, zero), jnp.where(first, zero, rows)], axis=0)


def join_heads(stacked):
    first = lax.broadcasted_iota(jnp.int32, (1, 2 * DH), 1) < DH
    return jnp.where(first, stacked[:TILE], stacked[TILE:])


def spread_bias(offsets_ref, tile_ref):
    for head in range(2):
        rows = jnp.broadcast_to(offsets_ref[head], (TILE, 4 * TILE))
        rolled = pltpu.roll(rows, 3 * TILE + 1, 1, stride=1, stride_axis=0)
        tile_ref[pl.ds(head * TILE, TILE), :] = rolled[:, : 3 * TILE]


def block_probs(query, key, bias, seg_q, seg_k):
    scores = lax.dot_general(query, key, NT, preferred_element_type=F32) + bias
    scores = jnp.where(seg_q == seg_k, scores, MASKED)
    expo = jnp.exp(scores - jnp.max(scores, axis=-1, keepdims=True))
    return expo * (1.0 / jnp.sum(expo, axis=-1, keepdims=True))


def attend_kernel(q_ref, k_ref, v_ref, offsets_ref, col_ref, row_ref, out_ref, tile_ref):
    @pl.when(pl.program_id(1) == 0)
    def _():
        spread_bias(offsets_ref, tile_ref)

    for start, low, keys, left in windows(q_ref.shape[0]):
        seg_q = col_ref[0, pl.ds(start, TILE), :]
        probs = block_probs(
            by_head(q_ref[pl.ds(start, TILE), :]),
            k_ref[pl.ds(low, keys), :],
            tile_ref[:, pl.ds(left, keys)],
            jnp.concatenate([seg_q, seg_q], axis=0),
            row_ref[0, :, pl.ds(low, keys)],
        )
        mixed = jnp.dot(
            probs.astype(BF16), v_ref[pl.ds(low, keys), :], preferred_element_type=F32
        )
        out_ref[pl.ds(start, TILE), :] = join_heads(mixed).astype(BF16)


def attend_back_kernel(
    q_ref, k_ref, v_ref, dm_ref, offsets_ref, col_ref, row_ref,
    dq_ref, dk_ref, dv_ref, dbias_ref, dk_sum, dv_sum, tile_ref,
):
    @pl.when(pl.program_id(1) == 0)
    def _():
        spread_bias(offsets_ref, tile_ref)
        dbias_ref[...] = jnp.zeros_like(dbias_ref)

    dk_sum[...] = jnp.zeros_like(dk_sum)
    dv_sum[...] = jnp.zeros_like(dv_sum)
    for start, low, keys, left in windows(q_ref.shape[0]):
        query = by_head(q_ref[pl.ds(start, TILE), :])
        grad = by_head(dm_ref[pl.ds(start, TILE), :])
        key = k_ref[pl.ds(low, keys), :]
        value = v_ref[pl.ds(low, keys), :]
        seg_q = col_ref[0, pl.ds(start, TILE), :]
        probs = block_probs(
            query, key, tile_ref[:, pl.ds(left, keys)],
            jnp.concatenate([seg_q, seg_q], axis=0), row_ref[0, :, pl.ds(low, keys)],
        )
        dprob = lax.dot_general(grad, value, NT, preferred_element_type=F32)
        centre = jnp.sum(probs * dprob, axis=-1, keepdims=True)
        dscore = (probs * (dprob - centre)).astype(BF16)
        wide = dscore.astype(F32)
        dbias_ref[0, :, pl.ds(left, keys)] += wide[:TILE]
        dbias_ref[1, :, pl.ds(left, keys)] += wide[TILE:]
        dq = jnp.dot(dscore, key, preferred_element_type=F32)
        dq_ref[pl.ds(start, TILE), :] = join_heads(dq).astype(BF16)
        dk_sum[pl.ds(low, keys), :] += lax.dot_general(
            dscore, query, TN, preferred_element_type=F32
        )
        dv_sum[pl.ds(low, keys), :] += lax.dot_general(
            probs.astype(BF16), grad, TN, preferred_element_type=F32
        )
    dk_ref[...] = dk_sum[...].astype(BF16)
    dv_ref[...] = dv_sum[...].astype(BF16)


def attend_specs(length):
    def lanes(offset):
        return pl.BlockSpec((length, 2 * DH), lambda pair, seq: (seq, pair + offset))

    bias = pl.BlockSpec((2, 1, 4 * TILE), lambda pair, seq: (pair, 0, 0))
    col = pl.BlockSpec((1, length, 1), lambda pair, seq: (seq, 0, 0))
    row = pl.BlockSpec((1, 1, length), lambda pair, seq: (seq, 0, 0))
    return lanes, bias, col, row


def attend(qkv, offsets, segments):
    sequences, length = segments.shape
    lanes, bias, col, row = attend_specs(length)
    width = H * DH
    steps = width // (2 * DH)
    work = sequences * H * length * 3 * TILE
    return pl.pallas_call(
        attend_kernel,
        grid=(steps, sequences),
        in_specs=[lanes(0), lanes(steps), lanes(2 * steps), bias, col, row],
        out_specs=lanes(0),
        out_shape=jax.ShapeDtypeStruct((sequences * length, width), BF16),
        scratch_shapes=[pltpu.VMEM((2 * TILE, 3 * TILE), F32)],
        name="attend",
        cost_estimate=pl.CostEstimate(
            flops=4 * work * 2 * DH, transcendentals=work, bytes_accessed=8 * qkv.size // 3
        ),
    )(qkv, qkv, qkv, offsets, segments[:, :, None], segments[:, None, :])


def attend_back(qkv, mixed_grad, offsets, segments):
    sequences, length = segments.shape
    lanes, bias, col, row = attend_specs(length)
    width = H * DH
    steps = width // (2 * DH)
    rows = sequences * length
    work = sequences * H * length * 3 * TILE
    flat = jax.ShapeDtypeStruct((rows, width), BF16)
    return pl.pallas_call(
        attend_back_kernel,
        grid=(steps, sequences),
        in_specs=[lanes(0), lanes(steps), lanes(2 * steps), lanes(0), bias, col, row],
        out_specs=[
            lanes(0), lanes(0), lanes(0),
            pl.BlockSpec((2, TILE, 3 * TILE), lambda pair, seq: (pair, 0, 0)),
        ],
        out_shape=[flat, flat, flat, jax.ShapeDtypeStruct((H, TILE, 3 * TILE), F32)],
        scratch_shapes=[
            pltpu.VMEM((length, 2 * DH), F32),
            pltpu.VMEM((length, 2 * DH), F32),
            pltpu.VMEM((2 * TILE, 3 * TILE), F32),
        ],
        name="attend_back",
        cost_estimate=pl.CostEstimate(
            flops=10 * work * 2 * DH, transcendentals=work, bytes_accessed=14 * qkv.size // 3
        ),
    )(qkv, qkv, qkv, mixed_grad, offsets, segments[:, :, None], segments[:, None, :])


def near_buckets(bucket_ids):
    centre = (bucket_ids.shape[0] + 1) // 2 - 1
    near = bucket_ids[centre - (2 * TILE - 1) : centre + 2 * TILE]
    return (near[:, None] == jnp.arange(BUCKETS, dtype=jnp.int32)[None, :]).astype(F32)


def offsets_of(table, bucket_ids):
    chosen = near_buckets(bucket_ids)
    offsets = jnp.dot(chosen, table.reshape(BUCKETS, H), precision=HIGHEST).T
    return jnp.pad(offsets, ((0, 0), (0, 1)))[:, None, :]


def table_grad_of(tile_sums, bucket_ids):
    chosen = near_buckets(bucket_ids)
    span = 4 * TILE
    rows = jnp.pad(tile_sums, ((0, 0), (0, 0), (TILE - 1, 0)))
    rows = jnp.pad(rows.reshape(H, -1), ((0, 0), (0, TILE))).reshape(H, TILE, span)
    offsets = jnp.sum(rows, axis=1)[:, : span - 1]
    return jnp.dot(chosen.T, offsets.T, precision=HIGHEST).reshape(-1)


def dot(left, right):
    return jnp.dot(left, right, preferred_element_type=F32)


def dot_nt(left, right):
    return lax.dot_general(left, right, NT, preferred_element_type=F32)


def dot_tn(left, right):
    return lax.dot_general(left, right, TN, preferred_element_type=F32)


def scale_of(rows):
    return lax.rsqrt(jnp.mean(rows * rows, axis=-1, keepdims=True) + EPSILON)


def norm_back(rows, scale, gain, upstream):
    weighted = upstream * gain
    inner = jnp.mean(rows * weighted, axis=-1, keepdims=True)
    rows_grad = scale * weighted - rows * (scale * scale * scale) * inner
    gain_grad = jnp.sum(rows * scale * upstream, axis=0)
    return rows_grad, gain_grad


def gated(gate_value, up_part):
    return jax.nn.gelu(gate_value, approximate=True) * up_part


def body(
    hidden_in, segment_ids, bucket_ids, norm1_gain, rel_bias, query_weight, key_weight,
    value_weight, output_weight, norm2_gain, gate_weight, up_weight, down_weight, out_grad,
):
    count = lax.axis_size("wide") * lax.axis_size("narrow")
    length, width = hidden_in.shape[2:]
    inner = gate_weight.shape[1]
    own, own_bias = norm1_gain.shape[0], rel_bias.shape[0]
    own_inner = down_weight.shape[0]

    small = jnp.zeros((own, 128), BF16)
    small = small.at[0, :own].set(norm1_gain).at[1, :own].set(norm2_gain)
    small = small.at[2, :own_bias].set(rel_bias)
    first = gather(jnp.concatenate([query_weight, key_weight, value_weight, small], axis=1))
    later = jnp.concatenate([output_weight, gate_weight, up_weight], axis=1)
    first, later = lax.optimization_barrier((first, later))
    later = gather(later)
    w_qkv = first[:, : 3 * width]
    smalls = first[:, 3 * width :].reshape(count, own, 128)
    gain_one = smalls[:, 0, :own].reshape(-1).astype(F32)
    gain_two = smalls[:, 1, :own].reshape(-1).astype(F32)
    table = smalls[:, 2, :own_bias].reshape(-1).astype(F32)
    segments = segment_ids.reshape(-1, length)
    rows = hidden_in.reshape(-1, width).astype(F32)
    out_rows = out_grad.reshape(-1, width)

    scale_one = scale_of(rows)
    normed = (rows * scale_one * gain_one).astype(BF16)
    qkv = dot(normed, w_qkv).astype(BF16)
    qkv, down_weight = lax.optimization_barrier((qkv, down_weight))
    w_down = gather(down_weight)
    offsets = offsets_of(table, bucket_ids)
    mixed, later = lax.optimization_barrier((attend(qkv, offsets, segments), later))
    w_output = later[:, :width]
    w_gate = later[:, width : width + inner]
    w_up = later[:, width + inner :]
    residual = rows + dot(mixed, w_output)
    scale_two = scale_of(residual)
    second = (residual * scale_two * gain_two).astype(BF16)
    gate_value = dot(second, w_gate)
    up_part = dot(second, w_up)
    hidden = gated(gate_value, up_part).astype(BF16)

    def scatter(order, *grads):
        return Sums([grad.astype(BF16) for grad in grads], count, order)

    down_sum = scatter((2, 1, 3, 4, 0), dot_tn(hidden, out_rows))
    hidden_grad = dot_nt(out_rows, w_down)
    _, pull_gate = jax.vjp(gated, gate_value, up_part)
    gate_grad, up_grad = pull_gate(hidden_grad)
    gate_grad, up_grad = gate_grad.astype(BF16), up_grad.astype(BF16)
    gate_sum = scatter((2, 0, 1, 3, 4), dot_tn(second, gate_grad))
    up_weight_grad = dot_tn(second, up_grad)
    up_grad = meet(up_grad, down_sum)
    second_grad = dot_nt(gate_grad, w_gate) + dot_nt(up_grad, w_up)
    residual_part, gain_two_grad = norm_back(residual, scale_two, gain_two, second_grad)
    residual_grad = out_rows.astype(F32) + residual_part
    branch_grad = residual_grad.astype(BF16)
    branch_grad = meet(branch_grad, gate_sum)
    up_sum = scatter((2, 0, 3, 1, 4), up_weight_grad, dot_tn(mixed, branch_grad))
    mixed_grad = dot_nt(branch_grad, w_output).astype(BF16)
    result = (residual + dot(hidden, w_down)).astype(BF16)
    mixed_grad, result = lax.optimization_barrier((mixed_grad, result))
    mixed_grad = meet(mixed_grad, down_sum)

    dq, dk, dv, tile_sums = attend_back(qkv, mixed_grad, offsets, segments)
    dv = meet(dv, down_sum, gate_sum, up_sum)
    half = width // 2
    key_weight_grad = dot_tn(normed, dk)
    value_sum = scatter((2, 0, 1, 3, 4), dot_tn(normed, dv), key_weight_grad[:, :half])
    query_sum = scatter((2, 1, 0, 3, 4), dot_tn(normed, dq), key_weight_grad[:, half:])
    dq = meet(dq, down_sum, gate_sum, up_sum)
    normed_grad = (
        dot_nt(dq, w_qkv[:, :width])
        + dot_nt(dk, w_qkv[:, width : 2 * width])
        + dot_nt(dv, w_qkv[:, 2 * width :])
    )
    rows_part, gain_one_grad = norm_back(rows, scale_one, gain_one, normed_grad)
    input_grad = (residual_grad + rows_part).astype(BF16)
    table_grad = table_grad_of(tile_sums, bucket_ids)

    def wide_rows(vector):
        return jnp.pad(vector.reshape(count, 1, -1), ((0, 0), (0, 0), (0, 128 - vector.size // count)))

    tiny = jnp.concatenate(
        [wide_rows(gain_one_grad), wide_rows(gain_two_grad), wide_rows(table_grad)], axis=1
    )
    tiny = jnp.pad(tiny, ((0, 0), (0, 5), (0, 0))).reshape(-1, 128)
    tiny = Sums([tiny], count, (2, 0, 1)).finish()
    up_out, value_key, query_key = up_sum.finish(), value_sum.finish(), query_sum.finish()
    return (
        result.reshape(hidden_in.shape),
        input_grad.reshape(hidden_in.shape),
        tiny[0, :own],
        tiny[2, :own_bias],
        query_key[:, :width],
        jnp.concatenate([value_key[:, width:], query_key[:, width:]], axis=1),
        value_key[:, :width],
        up_out[:, inner:],
        tiny[1, :own],
        gate_sum.finish(),
        up_out[:, :inner],
        down_sum.finish(),
    )


def solution(mesh):
    split, rows, tokens = P(AXES), P(AXES, None), P(None, AXES, None, None)
    in_specs = (
        tokens, P(None, AXES, None), P(), split, split, rows, rows, rows, rows,
        split, rows, rows, rows, tokens,
    )
    out_specs = (tokens, tokens, split, split, rows, rows, rows, rows, split, rows, rows, rows)
    return jax.shard_map(body, mesh=mesh, in_specs=in_specs, out_specs=out_specs, check_vma=False)
```

```python
import functools

import jax
import jax.numpy as jnp
from jax import lax
from jax.experimental import pallas as pl
from jax.experimental.pallas import tpu as pltpu
from jax.sharding import PartitionSpec as P

H = 16
DH = 64
BUCKETS = 32
AXES = ("wide", "narrow")
EPSILON = 1e-06
HIGHEST = lax.Precision.HIGHEST
MASKED = -1000000000.0
F32 = jnp.float32
BF16 = jnp.bfloat16
TILE = 128


def halve_order(count, first):
    bits = count.bit_length() - 1
    return [b for b in first if b < bits] + [b for b in range(bits) if b not in first]


def my_bit(bit):
    return (lax.axis_index(AXES) >> bit) & 1


def pairs(bit, count):
    return [(i, i ^ (1 << bit)) for i in range(count)]


class Sums:
    def __init__(self, grads, count, order):
        bits = count.bit_length() - 1
        self.count, self.order = count, halve_order(count, order)
        self.dims = list(range(bits - 1, -1, -1))
        self.exact = grads[0].dtype == F32
        self.parts = [grad.reshape((2,) * bits + (-1, grad.shape[-1])) for grad in grads]
        self.flying = None
        self.start()

    def half(self, axis, index):
        halves = [
            lax.dynamic_index_in_dim(part, index, axis, keepdims=False) for part in self.parts
        ]
        return halves[0] if len(halves) == 1 else jnp.concatenate(halves, axis=-1)

    def start(self):
        bit = self.order.pop(0)
        axis, mine = self.dims.index(bit), my_bit(bit)
        self.dims.pop(axis)
        keep, send = self.half(axis, mine), self.half(axis, 1 - mine)
        self.flying = [keep, lax.ppermute(send, AXES, pairs(bit, self.count))]

    def step(self):
        total = self.flying[0].astype(F32) + self.flying[1].astype(F32)
        self.parts = [total if self.exact or not self.order else total.astype(BF16)]
        self.flying = None
        if self.order:
            self.start()

    def finish(self):
        while self.flying is not None:
            self.step()
        return self.parts[0]


def meet(value, *sums):
    sums = [one for one in sums if one.flying is not None]
    value, got = lax.optimization_barrier((value, [one.flying[1] for one in sums]))
    for one, arrived in zip(sums, got):
        one.flying[1] = arrived
        one.step()
    return value


def gather(block):
    return lax.all_gather(block, AXES, axis=0, tiled=True)


MESH = pl.DeviceIdType.MESH
SLICES = 4


def column_slices(columns):
    tiles = columns // 128
    edges = [128 * (tiles * part // SLICES) for part in range(SLICES)] + [columns]
    return [(edges[part], edges[part + 1] - edges[part]) for part in range(SLICES)]


def gather_kernel(count, inner_count, *refs):
    arrays = (len(refs) - 3) // 2
    blocks, wholes = refs[:arrays], refs[arrays : 2 * arrays]
    local_sem, send_sem, recv_sem = refs[2 * arrays :]
    bits = count.bit_length() - 1
    core = inner_count.bit_length() - 1
    wide, narrow = lax.axis_index("wide"), lax.axis_index("narrow")
    me = wide * inner_count + narrow
    mine = [(me // (1 << bit)) % 2 for bit in range(bits)]

    def partner(bit):
        other = me + (1 - 2 * mine[bit]) * (1 << bit)
        return (other // inner_count, other % inner_count)

    def place(free):
        return tuple(
            slice(None) if bit in free else mine[bit] for bit in range(bits - 1, -1, -1)
        )

    barrier = pltpu.get_barrier_semaphore()
    for bit in range(bits):
        pl.semaphore_signal(barrier, inc=1, device_id=partner(bit), device_id_type=MESH)
    pl.semaphore_wait(barrier, bits)

    own = [
        pltpu.make_async_copy(block, whole.at[place(())], local_sem.at[i])
        for i, (block, whole) in enumerate(zip(blocks, wholes))
    ]
    for copy in own:
        copy.start()
    outer = list(range(bits - 1, core, -1))
    near = list(range(core))
    copies = {}
    for tick in range(SLICES + bits - 1):
        if tick == 1:
            for copy in own:
                copy.wait()
        for part in range(SLICES):
            step = tick - part
            if step < 0 or step >= bits:
                continue
            for i, (block, whole) in enumerate(zip(blocks, wholes)):
                flip = (part + i) % 2 == 1
                order = outer + (near[::-1] if flip else near) + [core]
                first, size = column_slices(block.shape[1])[part]
                columns = (slice(None), pl.ds(first, size))
                spot = place(order[:step]) + columns
                if step > 0:
                    copies[i, part, step - 1].wait_recv()
                copy = pltpu.make_async_remote_copy(
                    src_ref=block.at[columns] if step == 0 else whole.at[spot],
                    dst_ref=whole.at[spot],
                    send_sem=send_sem.at[i * SLICES + part, step],
                    recv_sem=recv_sem.at[i * SLICES + part, step],
                    device_id=partner(order[step]),
                    device_id_type=MESH,
                )
                copy.start()
                copies[i, part, step] = copy
    for (i, part, step), copy in copies.items():
        if step == bits - 1:
            copy.wait_recv()
    for copy in copies.values():
        copy.wait_send()


def gather_now(*blocks):
    count, inner_count = lax.axis_size(AXES), lax.axis_size("narrow")
    bits = count.bit_length() - 1
    lanes = (len(blocks) * SLICES, bits)
    wholes = pl.pallas_call(
        functools.partial(gather_kernel, count, inner_count),
        out_shape=[jax.ShapeDtypeStruct((2,) * bits + block.shape, block.dtype) for block in blocks],
        in_specs=[pl.BlockSpec(memory_space=pltpu.VMEM)] * len(blocks),
        out_specs=[pl.BlockSpec(memory_space=pl.ANY)] * len(blocks),
        scratch_shapes=[
            pltpu.SemaphoreType.DMA((len(blocks),)),
            pltpu.SemaphoreType.DMA(lanes),
            pltpu.SemaphoreType.DMA(lanes),
        ],
        compiler_params=pltpu.CompilerParams(collective_id=0, has_side_effects=True),
        name="gather_now",
    )(*blocks)
    return [
        whole.reshape((-1, block.shape[1])) for whole, block in zip(wholes, blocks)
    ]


def windows(length):
    out = []
    for start in range(0, length, TILE):
        low, high = max(0, start - TILE), min(length, start + 2 * TILE)
        out.append((start, low, high - low, low - start + TILE))
    return out


NT = (((1,), (1,)), ((), ()))
TN = (((0,), (0,)), ((), ()))


def by_head(rows):
    first = lax.broadcasted_iota(jnp.int32, (1, 2 * DH), 1) < DH
    zero = jnp.zeros_like(rows)
    return jnp.concatenate([jnp.where(first, rows, zero), jnp.where(first, zero, rows)], axis=0)


def join_heads(stacked):
    first = lax.broadcasted_iota(jnp.int32, (1, 2 * DH), 1) < DH
    return jnp.where(first, stacked[:TILE], stacked[TILE:])


def spread_bias(offsets_ref, tile_ref):
    for head in range(2):
        rows = jnp.broadcast_to(offsets_ref[head], (TILE, 4 * TILE))
        rolled = pltpu.roll(rows, 3 * TILE + 1, 1, stride=1, stride_axis=0)
        tile_ref[pl.ds(head * TILE, TILE), :] = rolled[:, : 3 * TILE]


def block_probs(query, key, bias, seg_q, seg_k):
    scores = lax.dot_general(query, key, NT, preferred_element_type=F32) + bias
    scores = jnp.where(seg_q == seg_k, scores, MASKED)
    expo = jnp.exp(scores - jnp.max(scores, axis=-1, keepdims=True))
    return expo * (1.0 / jnp.sum(expo, axis=-1, keepdims=True))


def attend_kernel(q_ref, k_ref, v_ref, offsets_ref, col_ref, row_ref, out_ref, tile_ref):
    @pl.when(pl.program_id(1) == 0)
    def _():
        spread_bias(offsets_ref, tile_ref)

    for start, low, keys, left in windows(q_ref.shape[0]):
        seg_q = col_ref[0, pl.ds(start, TILE), :]
        probs = block_probs(
            by_head(q_ref[pl.ds(start, TILE), :]),
            k_ref[pl.ds(low, keys), :],
            tile_ref[:, pl.ds(left, keys)],
            jnp.concatenate([seg_q, seg_q], axis=0),
            row_ref[0, :, pl.ds(low, keys)],
        )
        mixed = jnp.dot(
            probs.astype(BF16), v_ref[pl.ds(low, keys), :], preferred_element_type=F32
        )
        out_ref[pl.ds(start, TILE), :] = join_heads(mixed).astype(BF16)


def attend_back_kernel(
    q_ref, k_ref, v_ref, dm_ref, offsets_ref, col_ref, row_ref,
    dq_ref, dk_ref, dv_ref, dbias_ref, dk_sum, dv_sum, tile_ref,
):
    @pl.when(pl.program_id(1) == 0)
    def _():
        spread_bias(offsets_ref, tile_ref)
        dbias_ref[...] = jnp.zeros_like(dbias_ref)

    dk_sum[...] = jnp.zeros_like(dk_sum)
    dv_sum[...] = jnp.zeros_like(dv_sum)
    for start, low, keys, left in windows(q_ref.shape[0]):
        query = by_head(q_ref[pl.ds(start, TILE), :])
        grad = by_head(dm_ref[pl.ds(start, TILE), :])
        key = k_ref[pl.ds(low, keys), :]
        value = v_ref[pl.ds(low, keys), :]
        seg_q = col_ref[0, pl.ds(start, TILE), :]
        probs = block_probs(
            query, key, tile_ref[:, pl.ds(left, keys)],
            jnp.concatenate([seg_q, seg_q], axis=0), row_ref[0, :, pl.ds(low, keys)],
        )
        dprob = lax.dot_general(grad, value, NT, preferred_element_type=F32)
        centre = jnp.sum(probs * dprob, axis=-1, keepdims=True)
        dscore = (probs * (dprob - centre)).astype(BF16)
        wide = dscore.astype(F32)
        dbias_ref[0, :, pl.ds(left, keys)] += wide[:TILE]
        dbias_ref[1, :, pl.ds(left, keys)] += wide[TILE:]
        dq = jnp.dot(dscore, key, preferred_element_type=F32)
        dq_ref[pl.ds(start, TILE), :] = join_heads(dq).astype(BF16)
        dk_sum[pl.ds(low, keys), :] += lax.dot_general(
            dscore, query, TN, preferred_element_type=F32
        )
        dv_sum[pl.ds(low, keys), :] += lax.dot_general(
            probs.astype(BF16), grad, TN, preferred_element_type=F32
        )
    dk_ref[...] = dk_sum[...].astype(BF16)
    dv_ref[...] = dv_sum[...].astype(BF16)


def attend_specs(length):
    def lanes(offset):
        return pl.BlockSpec((length, 2 * DH), lambda pair, seq: (seq, pair + offset))

    bias = pl.BlockSpec((2, 1, 4 * TILE), lambda pair, seq: (pair, 0, 0))
    col = pl.BlockSpec((1, length, 1), lambda pair, seq: (seq, 0, 0))
    row = pl.BlockSpec((1, 1, length), lambda pair, seq: (seq, 0, 0))
    return lanes, bias, col, row


def attend(qkv, offsets, segments):
    sequences, length = segments.shape
    lanes, bias, col, row = attend_specs(length)
    width = H * DH
    steps = width // (2 * DH)
    work = sequences * H * length * 3 * TILE
    return pl.pallas_call(
        attend_kernel,
        grid=(steps, sequences),
        in_specs=[lanes(0), lanes(steps), lanes(2 * steps), bias, col, row],
        out_specs=lanes(0),
        out_shape=jax.ShapeDtypeStruct((sequences * length, width), BF16),
        scratch_shapes=[pltpu.VMEM((2 * TILE, 3 * TILE), F32)],
        name="attend",
        cost_estimate=pl.CostEstimate(
            flops=4 * work * 2 * DH, transcendentals=work, bytes_accessed=8 * qkv.size // 3
        ),
    )(qkv, qkv, qkv, offsets, segments[:, :, None], segments[:, None, :])


def attend_back(qkv, mixed_grad, offsets, segments):
    sequences, length = segments.shape
    lanes, bias, col, row = attend_specs(length)
    width = H * DH
    steps = width // (2 * DH)
    rows = sequences * length
    work = sequences * H * length * 3 * TILE
    flat = jax.ShapeDtypeStruct((rows, width), BF16)
    return pl.pallas_call(
        attend_back_kernel,
        grid=(steps, sequences),
        in_specs=[lanes(0), lanes(steps), lanes(2 * steps), lanes(0), bias, col, row],
        out_specs=[
            lanes(0), lanes(0), lanes(0),
            pl.BlockSpec((2, TILE, 3 * TILE), lambda pair, seq: (pair, 0, 0)),
        ],
        out_shape=[flat, flat, flat, jax.ShapeDtypeStruct((H, TILE, 3 * TILE), F32)],
        scratch_shapes=[
            pltpu.VMEM((length, 2 * DH), F32),
            pltpu.VMEM((length, 2 * DH), F32),
            pltpu.VMEM((2 * TILE, 3 * TILE), F32),
        ],
        name="attend_back",
        cost_estimate=pl.CostEstimate(
            flops=10 * work * 2 * DH, transcendentals=work, bytes_accessed=14 * qkv.size // 3
        ),
    )(qkv, qkv, qkv, mixed_grad, offsets, segments[:, :, None], segments[:, None, :])


def near_buckets(bucket_ids):
    centre = (bucket_ids.shape[0] + 1) // 2 - 1
    near = bucket_ids[centre - (2 * TILE - 1) : centre + 2 * TILE]
    return (near[:, None] == jnp.arange(BUCKETS, dtype=jnp.int32)[None, :]).astype(F32)


def offsets_of(table, bucket_ids):
    chosen = near_buckets(bucket_ids)
    offsets = jnp.dot(chosen, table.reshape(BUCKETS, H), precision=HIGHEST).T
    return jnp.pad(offsets, ((0, 0), (0, 1)))[:, None, :]


def table_grad_of(tile_sums, bucket_ids):
    chosen = near_buckets(bucket_ids)
    span = 4 * TILE
    rows = jnp.pad(tile_sums, ((0, 0), (0, 0), (TILE - 1, 0)))
    rows = jnp.pad(rows.reshape(H, -1), ((0, 0), (0, TILE))).reshape(H, TILE, span)
    offsets = jnp.sum(rows, axis=1)[:, : span - 1]
    return jnp.dot(chosen.T, offsets.T, precision=HIGHEST).reshape(-1)


def dot(left, right):
    return jnp.dot(left, right, preferred_element_type=F32)


def dot_nt(left, right):
    return lax.dot_general(left, right, NT, preferred_element_type=F32)


def dot_tn(left, right):
    return lax.dot_general(left, right, TN, preferred_element_type=F32)


def scale_of(rows):
    return lax.rsqrt(jnp.mean(rows * rows, axis=-1, keepdims=True) + EPSILON)


def norm_back(rows, scale, gain, upstream):
    weighted = upstream * gain
    inner = jnp.mean(rows * weighted, axis=-1, keepdims=True)
    rows_grad = scale * weighted - rows * (scale * scale * scale) * inner
    gain_grad = jnp.sum(rows * scale * upstream, axis=0)
    return rows_grad, gain_grad


def gated(gate_value, up_part):
    return jax.nn.gelu(gate_value, approximate=True) * up_part


def body(
    hidden_in, segment_ids, bucket_ids, norm1_gain, rel_bias, query_weight, key_weight,
    value_weight, output_weight, norm2_gain, gate_weight, up_weight, down_weight, out_grad,
):
    count = lax.axis_size("wide") * lax.axis_size("narrow")
    length, width = hidden_in.shape[2:]
    inner = gate_weight.shape[1]
    own, own_bias = norm1_gain.shape[0], rel_bias.shape[0]
    own_inner = down_weight.shape[0]

    small = jnp.zeros((own, 128), BF16)
    small = small.at[0, :own].set(norm1_gain).at[1, :own].set(norm2_gain)
    small = small.at[2, :own_bias].set(rel_bias)
    later = gather(jnp.concatenate([output_weight, gate_weight, up_weight], axis=1))
    first, w_down = gather_now(
        jnp.concatenate([query_weight, key_weight, value_weight, small], axis=1), down_weight
    )
    w_qkv = first[:, : 3 * width]
    smalls = first[:, 3 * width :].reshape(count, own, 128)
    gain_one = smalls[:, 0, :own].reshape(-1).astype(F32)
    gain_two = smalls[:, 1, :own].reshape(-1).astype(F32)
    table = smalls[:, 2, :own_bias].reshape(-1).astype(F32)
    segments = segment_ids.reshape(-1, length)
    rows = hidden_in.reshape(-1, width).astype(F32)
    out_rows = out_grad.reshape(-1, width)

    scale_one = scale_of(rows)
    normed = (rows * scale_one * gain_one).astype(BF16)
    qkv = dot(normed, w_qkv).astype(BF16)
    offsets = offsets_of(table, bucket_ids)
    mixed, later = lax.optimization_barrier((attend(qkv, offsets, segments), later))
    w_output = later[:, :width]
    w_gate = later[:, width : width + inner]
    w_up = later[:, width + inner :]
    residual = rows + dot(mixed, w_output)
    scale_two = scale_of(residual)
    second = (residual * scale_two * gain_two).astype(BF16)
    gate_value = dot(second, w_gate)
    up_part = dot(second, w_up)
    hidden = gated(gate_value, up_part).astype(BF16)

    def scatter(order, *grads):
        return Sums([grad.astype(BF16) for grad in grads], count, order)

    down_sum = scatter((2, 1, 3, 4, 0), dot_tn(hidden, out_rows))
    hidden_grad = dot_nt(out_rows, w_down)
    _, pull_gate = jax.vjp(gated, gate_value, up_part)
    gate_grad, up_grad = pull_gate(hidden_grad)
    gate_grad, up_grad = gate_grad.astype(BF16), up_grad.astype(BF16)
    gate_sum = scatter((2, 0, 1, 3, 4), dot_tn(second, gate_grad))
    up_weight_grad = dot_tn(second, up_grad)
    up_grad = meet(up_grad, down_sum)
    second_grad = dot_nt(gate_grad, w_gate) + dot_nt(up_grad, w_up)
    residual_part, gain_two_grad = norm_back(residual, scale_two, gain_two, second_grad)
    residual_grad = out_rows.astype(F32) + residual_part
    branch_grad = residual_grad.astype(BF16)
    branch_grad = meet(branch_grad, gate_sum)
    up_sum = scatter((2, 0, 3, 1, 4), up_weight_grad, dot_tn(mixed, branch_grad))
    mixed_grad = dot_nt(branch_grad, w_output).astype(BF16)
    result = (residual + dot(hidden, w_down)).astype(BF16)
    mixed_grad, result = lax.optimization_barrier((mixed_grad, result))
    mixed_grad = meet(mixed_grad, down_sum)

    dq, dk, dv, tile_sums = attend_back(qkv, mixed_grad, offsets, segments)
    dv = meet(dv, down_sum, gate_sum, up_sum)
    half = width // 2
    key_weight_grad = dot_tn(normed, dk)
    value_sum = scatter((2, 0, 1, 3, 4), dot_tn(normed, dv), key_weight_grad[:, :half])
    query_sum = scatter((2, 1, 0, 3, 4), dot_tn(normed, dq), key_weight_grad[:, half:])
    dq = meet(dq, down_sum, gate_sum, up_sum)
    normed_grad = (
        dot_nt(dq, w_qkv[:, :width])
        + dot_nt(dk, w_qkv[:, width : 2 * width])
        + dot_nt(dv, w_qkv[:, 2 * width :])
    )
    rows_part, gain_one_grad = norm_back(rows, scale_one, gain_one, normed_grad)
    input_grad = (residual_grad + rows_part).astype(BF16)
    table_grad = table_grad_of(tile_sums, bucket_ids)

    def wide_rows(vector):
        return jnp.pad(vector.reshape(count, 1, -1), ((0, 0), (0, 0), (0, 128 - vector.size // count)))

    tiny = jnp.concatenate(
        [wide_rows(gain_one_grad), wide_rows(gain_two_grad), wide_rows(table_grad)], axis=1
    )
    tiny = jnp.pad(tiny, ((0, 0), (0, 5), (0, 0))).reshape(-1, 128)
    tiny = Sums([tiny], count, (2, 0, 1)).finish()
    up_out, value_key, query_key = up_sum.finish(), value_sum.finish(), query_sum.finish()
    return (
        result.reshape(hidden_in.shape),
        input_grad.reshape(hidden_in.shape),
        tiny[0, :own],
        tiny[2, :own_bias],
        query_key[:, :width],
        jnp.concatenate([value_key[:, width:], query_key[:, width:]], axis=1),
        value_key[:, :width],
        up_out[:, inner:],
        tiny[1, :own],
        gate_sum.finish(),
        up_out[:, :inner],
        down_sum.finish(),
    )


def solution(mesh):
    split, rows, tokens = P(AXES), P(AXES, None), P(None, AXES, None, None)
    in_specs = (
        tokens, P(None, AXES, None), P(), split, split, rows, rows, rows, rows,
        split, rows, rows, rows, tokens,
    )
    out_specs = (tokens, tokens, split, split, rows, rows, rows, rows, split, rows, rows, rows)
    return jax.shard_map(body, mesh=mesh, in_specs=in_specs, out_specs=out_specs, check_vma=False)
```
